32 devices in a mesh: rows: 16 (over z, y, x), layer: 2 (over core).
Axes of the slice: x: 2, y: 2, z: 4, core: 2. Of those that a mesh axis runs over, the one named last changes fastest.
Arguments:
- grads: bfloat16 [2, 2048, 8192], P('layer', 'rows'), may hold values from -180 to 180
- momentum: float32 [2, 2048, 8192], P('layer', 'rows'), may hold values from -6 to 6
- weights: float32 [2, 2048, 8192], P('layer', 'rows'), may hold values from -1.5 to 1.5
Outputs:
- new_weights: float32 [2, 2048, 8192], P('layer', 'rows')
- new_momentum: float32 [2, 2048, 8192], P('layer', 'rows')
The draws below stay inside these ranges and needn't reach their ends.
All inputs are finite; a program needn't handle non-finite values.
Results may differ from the reference program's by a relative error of at most 0.0003.
Values sent between devices are 32-bit elements; how exact they have to be, the bound alone decides.
A program may use at most 128 MiB of HBM per device.

```python
import math
import jax
import jax.numpy as jnp
from jax import lax

LATENT = 2048
HEADS = 32
HD = 256
ITERS = 5
LAYERS = 2


def draw_grads(key, part):
    first_key, second_key, third_key = jax.random.split(jax.random.fold_in(key, 17), 3)
    shape = (LAYERS, LATENT, HEADS * HD)
    base = jnp.clip(jax.random.normal(first_key, shape, jnp.float32), -6.0, 6.0)
    row_scale = jnp.exp(jax.random.uniform(second_key, (LAYERS, LATENT, 1), jnp.float32, 0.0, 1.0) * 0.5 * math.log(10.0))
    column_scale = jnp.exp(jax.random.uniform(third_key, (LAYERS, 1, HEADS * HD), jnp.float32, 0.0, 1.0) * 0.5 * math.log(10.0))
    row_place = jnp.arange(LATENT, dtype=jnp.float32)[None, :, None] / LATENT
    layer_place = jnp.arange(LAYERS, dtype=jnp.float32)[:, None, None] / max(LAYERS - 1, 1)
    ramp = jnp.exp(0.5 * math.log(3.0) * (row_place + layer_place))
    return (base * row_scale * column_scale * ramp).astype(jnp.bfloat16)


def steps_of(own_key, dims, cuts, smallest, top_value):
    loudness = 1.0
    for dim, shards_of in cuts:
        draws = jax.random.uniform(jax.random.fold_in(jax.random.fold_in(own_key, 6), dim), (shards_of,), jnp.float32, smallest / len(cuts), top_value / len(cuts))
        loudness = loudness * jnp.repeat(jnp.exp(draws), dims[dim] // shards_of).reshape((-1,) + (1,) * (len(dims) - 1 - dim))
    return loudness


def scatter_about(key, dims, deviation, bound, cuts=(), kind=jnp.bfloat16):
    values = deviation * jax.random.normal(key, dims, jnp.float32)
    if cuts:
        values = values * steps_of(key, dims, cuts, -0.22, 0.18)
    return jnp.clip(values, -bound, bound).astype(kind)


def setup_inputs(seed: int = 0) -> dict:
    key_list = jax.random.split(jax.random.key(seed), 4)
    return {
        "grads": draw_grads(jax.random.fold_in(key_list[3], 71), 0),
        "momentum": scatter_about(key_list[1], (LAYERS, LATENT, HEADS * HD), 0.5, 6.0, ((0, 2), (1, 16)), jnp.float32),
        "weights": scatter_about(key_list[2], (LAYERS, LATENT, HEADS * HD), 0.1, 1.5, ((0, 2), (1, 16)), jnp.float32),
    }


coef_a = 3.4445
coef_b = -4.775
coef_c = 2.0315

def newton_schulz(blocks):
    first = jnp.einsum('kri,krj->kij', blocks, blocks, precision=lax.Precision.HIGHEST)
    norm = jnp.sqrt(jnp.trace(first, axis1=1, axis2=2))[:, None, None] + 1e-07
    current = blocks / norm
    gram = first / (norm * norm)
    for sweep in range(ITERS):
        if sweep > 0:
            gram = jnp.einsum('kri,krj->kij', current, current, precision=lax.Precision.HIGHEST)
        square = jnp.einsum('kij,kjl->kil', gram, gram, precision=lax.Precision.HIGHEST)
        poly = coef_b * gram + coef_c * square
        current = coef_a * current + jnp.einsum('kri,kij->krj', current, poly, precision=lax.Precision.HIGHEST)
    return current

def one_layer(update):
    blocks = update.reshape(LATENT, HEADS, HD).transpose(1, 0, 2)
    result = newton_schulz(blocks)
    return result.transpose(1, 0, 2).reshape(LATENT, HEADS * HD)

def reference(grads, momentum, weights):
    gradient = grads.astype(jnp.float32)
    total = jnp.sum(gradient * gradient)
    limit = 0.5 * math.sqrt(float(LAYERS * LATENT * HEADS * HD))
    factor = jnp.minimum(1.0, limit / (jnp.sqrt(total) + 1e-06))
    clipped = factor * gradient
    new_momentum = 0.95 * momentum + clipped
    update = clipped + 0.95 * new_momentum
    ortho = lax.map(one_layer, update)
    scale = 0.2 * math.sqrt(float(max(LATENT, HD)))
    new_weights = weights - 0.5 * (scale * ortho + 0.1 * weights)
    return (new_weights, new_momentum)
```

```python
import functools
import math

import jax
import jax.numpy as jnp
from jax import lax
from jax.experimental import pallas as pl
from jax.experimental.pallas import tpu as pltpu
from jax.sharding import PartitionSpec as P

HD = 256
ITERS = 5

coef_a = 3.4445
coef_b = -4.775
coef_c = 2.0315
momentum_decay = 0.95
learn_rate = 0.5
weight_decay = 0.1

HIGHEST = lax.Precision.HIGHEST
MESH = pl.DeviceIdType.MESH


def mm(a, b):
    return jnp.dot(a, b, precision=HIGHEST, preferred_element_type=jnp.float32)


def split(x):
    high = x.astype(jnp.bfloat16)
    low = (x - high.astype(jnp.float32)).astype(jnp.bfloat16)
    return high, low


def polynomial(gram):
    row = lax.broadcasted_iota(jnp.int32, (HD, HD), 0)
    col = lax.broadcasted_iota(jnp.int32, (HD, HD), 1)
    eye = jnp.where(row == col, 1.0, 0.0).astype(jnp.float32)
    trace = jnp.sum(jnp.sum(gram * eye, axis=0, keepdims=True), axis=1, keepdims=True)
    norm = jnp.sqrt(trace) + 1e-07
    a = gram / (norm * norm)
    q = None
    for sweep in range(ITERS):
        p = coef_a * eye + (coef_b * a + coef_c * mm(a, a))
        q = p if q is None else mm(q, p)
        if sweep < ITERS - 1:
            a = mm(mm(a, p), p)
    return q / norm


def dot(a, b):
    return jnp.dot(a, b, preferred_element_type=jnp.float32)


def across(a, b):
    return lax.dot_general(a, b, (((0,), (0,)), ((), ())), preferred_element_type=jnp.float32)


HALF = HD // 2
EDGE = 8
FIRST = HALF + EDGE
PIECES = FIRST + HALF
A = pl.ds(0, FIRST)
B = pl.ds(FIRST, HALF)


def grid_of_half():
    return lax.broadcasted_iota(jnp.int32, (HALF, HALF), 0), lax.broadcasted_iota(jnp.int32, (HALF, HALF), 1)


def store_packed(ref, lower, upper, diagonal, off):
    row, col = grid_of_half()
    ref[pl.ds(0, HALF), :] = jnp.where(row >= col, lower, upper)
    edge = jnp.sum(jnp.where(row == col, diagonal, 0.0), axis=0, keepdims=True)
    ref[pl.ds(HALF, EDGE), :] = jnp.broadcast_to(edge, (EDGE, HALF))
    ref[B, :] = off


def store_gram(ref, x):
    high = x.astype(jnp.bfloat16)
    rest = x - high.astype(jnp.float32)
    middle = rest.astype(jnp.bfloat16)
    low = (rest - middle.astype(jnp.float32)).astype(jnp.bfloat16)
    both = jnp.concatenate([high, middle], axis=0)
    even = across(both, both)
    half = across(jnp.concatenate([high, high], axis=0), jnp.concatenate([middle, low], axis=0))
    row, col = grid_of_half()
    h0, h1 = half[:HALF, :HALF], half[HALF:, HALF:]
    turned = jnp.where(row <= col, h0, h1).T
    e0, e1 = even[:HALF, :HALF], even[HALF:, HALF:]
    off = even[:HALF, HALF:] + (half[:HALF, HALF:] + half[HALF:, :HALF].T)
    store_packed(ref, e0 + h0 + turned, e1 + h1 + turned, e1 + 2.0 * h1, off)


def unpack(ref):
    row, col = grid_of_half()
    block, edge, off = ref[pl.ds(0, HALF), :], ref[pl.ds(HALF, 1), :], ref[B, :]
    turned = block.T
    first = jnp.where(row >= col, block, turned)
    second = jnp.where(row < col, block, jnp.where(row > col, turned, edge))
    return jnp.concatenate(
        [jnp.concatenate([first, off], axis=1), jnp.concatenate([off.T, second], axis=1)], axis=0
    )


def toggle(index, flips, count):
    out, bit = 0, 1
    while bit < count:
        out = out + (index // bit + flips // bit) % 2 * bit
        bit *= 2
    return out


def exchange_kernel(
    devices, layers, limit, scale, g_hbm, m_hbm, w_hbm, new_w_ref, new_m_ref,
    g_ref, m_ref, w_ref, squares, mine, own, ra, ra2, rb, rb2, zr, q,
    square_send, square_recv, a1_send, a1_recv, b1_send, b1_recv, a2_send, a2_recv, b2_send, b2_recv,
    z_send, z_recv, ay_send, ay_recv, ax_send, ax_recv, bx_send, bx_recv, by_send, by_recv,
    qz_send, qz_recv, load_sem,
):
    rows, width = g_ref.shape
    heads = width // HD
    depth = devices // 4
    groups = heads // devices
    everyone = devices * layers
    me = lax.axis_index("rows")
    layer = lax.axis_index("layer")
    flat = me * layers + layer
    z, y, x = me // 4, me // 2 % 2, me % 2
    peer_x = z * 4 + y * 2 + (1 - x)
    peer_y = z * 4 + (1 - y) * 2 + x
    parts = load_sem.shape[0] - 2
    span = width // parts

    def load_g(i):
        cols = pl.ds(i * span, span)
        return pltpu.make_async_copy(g_hbm.at[:, cols], g_ref.at[:, cols], load_sem.at[2 + i])

    load_m = pltpu.make_async_copy(m_hbm, m_ref, load_sem.at[0])
    load_w = pltpu.make_async_copy(w_hbm, w_ref, load_sem.at[1])
    for i in range(parts):
        load_g(i).start()
    load_m.start()
    load_w.start()
    barrier = pltpu.get_barrier_semaphore()

    @pl.loop(1, everyone)
    def _(k):
        peer = (flat + k) % everyone
        pl.semaphore_signal(
            barrier, inc=1, device_id={"rows": peer // layers, "layer": peer % layers}, device_id_type=MESH
        )

    def columns_of(h):
        return pl.ds(pl.multiple_of(h * HD, HD), HD)

    def add_squares(h, acc):
        g = g_ref[:, columns_of(h)].astype(jnp.float32)
        return acc + (g * g).reshape(rows // 8, 8, HD).sum(axis=0)

    acc = jnp.zeros((8, HD), jnp.float32)
    for i in range(parts):
        load_g(i).wait()
        acc = lax.fori_loop(i * (heads // parts), (i + 1) * (heads // parts), add_squares, acc)
    part = acc[:, :128] + acc[:, 128:]
    mine[...] = part
    squares[flat] = part
    pl.semaphore_wait(barrier, everyone - 1)

    def square_copy(k):
        peer = (flat + k) % everyone
        return pltpu.make_async_remote_copy(
            src_ref=mine,
            dst_ref=squares.at[flat],
            send_sem=square_send.at[k],
            recv_sem=square_recv.at[k],
            device_id={"rows": peer // layers, "layer": peer % layers},
            device_id_type=MESH,
        )

    @pl.loop(1, everyone)
    def _(k):
        square_copy(k).start()

    @pl.loop(1, everyone)
    def _(k):
        square_copy(k).wait_recv()

    total = jnp.sum(squares[...], axis=0)
    total = jnp.sum(jnp.sum(total, axis=0, keepdims=True), axis=1, keepdims=True)
    factor = jnp.minimum(1.0, limit / (jnp.sqrt(total) + 1e-06))
    load_m.wait()
    load_w.wait()

    def layer_of(k):
        return toggle(z, k, depth)

    def head_of(j, t, kind):
        owner = t * 4 + (y + kind % 2) % 2 * 2 + (x + kind // 2) % 2
        return owner * groups + j

    def send(src, dst, send_sem, recv_sem, device):
        return pltpu.make_async_remote_copy(
            src_ref=src, dst_ref=dst, send_sem=send_sem, recv_sem=recv_sem,
            device_id={"rows": device}, device_id_type=MESH,
        )

    def a1(j, t, dy):
        return send(own.at[j, t, 2 + dy, A], ra.at[j, t, dy], a1_send.at[j, t, dy], a1_recv.at[j, t, dy], peer_x)

    def b1(j, t, dx):
        return send(own.at[j, t, 2 * dx + 1, B], rb.at[j, t, dx], b1_send.at[j, t, dx], b1_recv.at[j, t, dx], peer_y)

    def a2(j, t):
        return send(own.at[j, t, 1, A], ra2.at[j, t], a2_send.at[j, t], a2_recv.at[j, t], peer_y)

    def b2(j, t):
        return send(own.at[j, t, 2, B], rb2.at[j, t], b2_send.at[j, t], b2_recv.at[j, t], peer_x)

    def zc(j, k):
        t = layer_of(k)
        return send(own.at[j, t, 0], zr.at[j, z], z_send.at[j, k], z_recv.at[j, k], t * 4 + y * 2 + x)

    def qz(j, k):
        t = layer_of(k)
        return send(q.at[j, z, 0], q.at[j, z, 0], qz_send.at[j, k], qz_recv.at[j, k], t * 4 + y * 2 + x)

    def ay(j, t):
        return send(q.at[j, t, 0, A], q.at[j, t, 1, A], ay_send.at[j, t], ay_recv.at[j, t], peer_y)

    def ax(j, t, dy):
        return send(q.at[j, t, dy, A], q.at[j, t, 2 + dy, A], ax_send.at[j, t, dy], ax_recv.at[j, t, dy], peer_x)

    def bx(j, t):
        return send(q.at[j, t, 0, B], q.at[j, t, 2, B], bx_send.at[j, t], bx_recv.at[j, t], peer_x)

    def by(j, t, dx):
        return send(
            q.at[j, t, 2 * dx, B], q.at[j, t, 2 * dx + 1, B], by_send.at[j, t, dx], by_recv.at[j, t, dx], peer_y
        )

    def grams(j, kind):
        for k in reversed(range(depth)):
            t = layer_of(k)
            cols = columns_of(head_of(j, t, kind))
            clipped = factor * g_ref[:, cols].astype(jnp.float32)
            new_momentum = momentum_decay * m_ref[:, cols] + clipped
            new_m_ref[:, cols] = new_momentum
            store_gram(own.at[j, t, kind], clipped + momentum_decay * new_momentum)

    def first_sends(j, kind):
        for k in reversed(range(depth)):
            t = layer_of(k)
            pl.when(kind // 2 == 1)(lambda: a1(j, t, kind % 2).start())
            pl.when(kind % 2 == 1)(lambda: b1(j, t, kind // 2).start())

    def second_send(j, k):
        t = layer_of(k)
        a1(j, t, 1).wait_recv()
        own[j, t, 1, A, :] += ra[j, t, 1]
        a2(j, t).start()
        b1(j, t, 1).wait_recv()
        own[j, t, 2, B, :] += rb[j, t, 1]
        b2(j, t).start()

    def third_send(j, k):
        t = layer_of(k)
        a1(j, t, 0).wait_recv()
        b1(j, t, 0).wait_recv()
        a2(j, t).wait_recv()
        b2(j, t).wait_recv()
        a = own[j, t, 0, A, :] + (ra[j, t, 0] + ra2[j, t])
        b = own[j, t, 0, B, :] + (rb[j, t, 0] + rb2[j, t])
        if k == 0:
            zr[j, t, A, :] = a
            zr[j, t, B, :] = b
        else:
            own[j, t, 0, A, :] = a
            own[j, t, 0, B, :] = b
            zc(j, k).start()

    def solve(j):
        for k in range(1, depth):
            zc(j, k).wait_recv()
        own[j, z, 0] = jnp.sum(zr[j], axis=0)
        p = polynomial(unpack(own.at[j, z, 0]))
        store_packed(q.at[j, z, 0], p[:HALF, :HALF], p[HALF:, HALF:], p[HALF:, HALF:], p[:HALF, HALF:])

    def share(j):
        for k in reversed(range(1, depth)):
            qz(j, k).start()

    def pass_on(j, k):
        t = layer_of(k)
        if not (isinstance(k, int) and k == 0):
            qz(j, k).wait_recv()
        ay(j, t).start()
        bx(j, t).start()
        ax(j, t, 0).start()
        by(j, t, 0).start()

    def pass_far(j, k):
        t = layer_of(k)
        ay(j, t).wait_recv()
        ax(j, t, 1).start()
        bx(j, t).wait_recv()
        by(j, t, 1).start()

    def finish(j, k):
        t = layer_of(k)
        by(j, t, 0).wait_recv()
        by(j, t, 1).wait_recv()
        ax(j, t, 0).wait_recv()
        ax(j, t, 1).wait_recv()
        for kind in range(4):
            cols = columns_of(head_of(j, t, kind))
            q_high, q_low = split(unpack(q.at[j, t, kind]))
            update = factor * g_ref[:, cols].astype(jnp.float32) + momentum_decay * new_m_ref[:, cols]
            high, low = split(update)
            ortho = dot(high, q_high) + (dot(low, q_high) + dot(high, q_low))
            w = w_ref[:, cols]
            new_w_ref[:, cols] = w - learn_rate * (scale * ortho + weight_decay * w)

    def gather(j):
        @pl.loop(0, 4)
        def _(i):
            grams(j, 3 - i)
            first_sends(j, 3 - i)

    def answer(j):
        solve(j)
        share(j)
        pass_on(j, 0)

    last = groups - 1
    far = list(reversed(range(depth)))
    gather(0)
    for j in range(groups):
        for k in far:
            second_send(j, k)
        if j < last:
            gather(j + 1)
        if j > 0:
            answer(j - 1)
        for k in far:
            third_send(j, k)
        if j > 0:
            for k in range(1, depth):
                pass_on(j - 1, k)
                pass_far(j - 1, k - 1)
    answer(last)
    if last > 0:
        for j in range(last):
            pass_far(j, depth - 1)

    @pl.loop(0, depth)
    def _(k):
        @pl.when(k + 1 < depth)
        def _():
            pass_on(last, k + 1)

        pass_far(last, k)
        for j in range(last):
            finish(j, k)

    @pl.loop(0, depth)
    def _(k):
        finish(last, k)

    @pl.loop(0, groups)
    def _(j):
        @pl.loop(0, depth)
        def _(k):
            for c in (a1(j, k, 0), a1(j, k, 1), b1(j, k, 0), b1(j, k, 1), a2(j, k), b2(j, k)):
                c.wait_send()
            for c in (ay(j, k), ax(j, k, 0), ax(j, k, 1), bx(j, k), by(j, k, 0), by(j, k, 1)):
                c.wait_send()

        @pl.loop(1, depth)
        def _(k):
            zc(j, k).wait_send()
            qz(j, k).wait_send()

    @pl.loop(1, everyone)
    def _(k):
        square_copy(k).wait_send()


def exchange(gradient, momentum, weights, devices, layers, limit, scale):
    rows, width = gradient.shape
    heads = width // HD
    depth = devices // 4
    groups = heads // devices
    everyone = devices * layers
    vmem = lambda *shape: pltpu.VMEM(shape, jnp.float32)
    pair = lambda *shape: [pltpu.SemaphoreType.DMA(shape)] * 2
    one, two = (groups, depth), (groups, depth, 2)
    return pl.pallas_call(
        functools.partial(exchange_kernel, devices, layers, limit, scale),
        out_shape=(
            jax.ShapeDtypeStruct((rows, width), jnp.float32),
            jax.ShapeDtypeStruct((rows, width), jnp.float32),
        ),
        in_specs=[pl.BlockSpec(memory_space=pl.ANY)] * 3,
        out_specs=(pl.BlockSpec(memory_space=pltpu.VMEM), pl.BlockSpec(memory_space=pltpu.VMEM)),
        scratch_shapes=[
            pltpu.VMEM((rows, width), gradient.dtype),
            vmem(rows, width),
            vmem(rows, width),
            vmem(everyone, 8, 128),
            vmem(8, 128),
            vmem(groups, depth, 4, PIECES, HALF),
            vmem(groups, depth, 2, FIRST, HALF),
            vmem(groups, depth, FIRST, HALF),
            vmem(groups, depth, 2, HALF, HALF),
            vmem(groups, depth, HALF, HALF),
            vmem(groups, depth, PIECES, HALF),
            vmem(groups, depth, 4, PIECES, HALF),
            *pair(everyone),
            *pair(*two), *pair(*two), *pair(*one), *pair(*one), *pair(*one),
            *pair(*one), *pair(*two), *pair(*one), *pair(*two), *pair(*one),
            pltpu.SemaphoreType.DMA((2 + math.gcd(heads, 4),)),
        ],
        compiler_params=pltpu.CompilerParams(
            collective_id=0, has_side_effects=True, vmem_limit_bytes=56 * 1024 * 1024
        ),
    )(gradient, momentum, weights)


def body(grads, momentum, weights):
    devices, layers = lax.axis_size("rows"), lax.axis_size("layer")
    rows, width = grads.shape[1:]
    limit = 0.5 * math.sqrt(float(layers * devices * rows * width))
    scale = 0.2 * math.sqrt(float(max(devices * rows, HD)))
    new_weights, new_momentum = exchange(grads[0], momentum[0], weights[0], devices, layers, limit, scale)
    return (new_weights[None], new_momentum[None])


def shared_body(grads, momentum, weights):
    devices = lax.axis_size("rows")
    rows, width = grads.shape[1:]
    heads = width // HD
    gradient = grads[0].astype(jnp.float32)
    total = lax.psum(jnp.sum(gradient * gradient), ("rows", "layer"))
    limit = 0.5 * math.sqrt(float(lax.axis_size("layer") * devices * rows * width))
    factor = jnp.minimum(1.0, limit / (jnp.sqrt(total) + 1e-06))
    clipped = factor * gradient
    new_momentum = momentum_decay * momentum[0] + clipped
    update = clipped + momentum_decay * new_momentum
    sharers = devices // heads
    part = rows // sharers
    head_major = update.reshape(rows, heads, HD).transpose(1, 0, 2)
    outgoing = jnp.concatenate([head_major] * sharers, axis=0)
    pieces = lax.all_to_all(outgoing, "rows", split_axis=0, concat_axis=1, tiled=True)
    x = pieces[0]
    gram = lax.dot_general(x, x, (((0,), (0,)), ((), ())), precision=HIGHEST)
    result = mm(x, polynomial(gram))
    side = lax.axis_index("rows") // heads
    shares = result.reshape(devices, sharers, part, HD)
    chosen = lax.dynamic_index_in_dim(shares, side, 1, keepdims=False)
    returned = lax.all_to_all(chosen, "rows", split_axis=0, concat_axis=0, tiled=True)
    returned = returned.reshape(sharers, heads, part, HD).transpose(0, 2, 1, 3).reshape(rows, width)
    scale = 0.2 * math.sqrt(float(max(devices * rows, HD)))
    new_weights = weights[0] - learn_rate * (scale * returned + weight_decay * weights[0])
    return (new_weights[None], new_momentum[None])


def solution(mesh):
    placed = P("layer", "rows", None)

    def step(grads, momentum, weights):
        heads = grads.shape[2] // HD
        devices = mesh.shape["rows"]
        depth = devices // 4
        direct = heads % devices == 0 and devices == 4 * depth and depth & (depth - 1) == 0
        chosen = body if direct else shared_body
        return jax.shard_map(
            chosen, mesh=mesh, in_specs=(placed,) * 3, out_specs=(placed, placed), check_vma=False
        )(grads, momentum, weights)

    return step
```

```python
import functools
import math

import jax
import jax.numpy as jnp
from jax import lax
from jax.experimental import pallas as pl
from jax.experimental.pallas import tpu as pltpu
from jax.sharding import PartitionSpec as P

HD = 256
ITERS = 5

coef_a = 3.4445
coef_b = -4.775
coef_c = 2.0315
momentum_decay = 0.95
learn_rate = 0.5
weight_decay = 0.1

HIGHEST = lax.Precision.HIGHEST
MESH = pl.DeviceIdType.MESH


def mm(a, b):
    return jnp.dot(a, b, precision=HIGHEST, preferred_element_type=jnp.float32)


def split(x):
    high = x.astype(jnp.bfloat16)
    low = (x - high.astype(jnp.float32)).astype(jnp.bfloat16)
    return high, low


def polynomial(gram):
    row = lax.broadcasted_iota(jnp.int32, (HD, HD), 0)
    col = lax.broadcasted_iota(jnp.int32, (HD, HD), 1)
    eye = jnp.where(row == col, 1.0, 0.0).astype(jnp.float32)
    trace = jnp.sum(jnp.sum(gram * eye, axis=0, keepdims=True), axis=1, keepdims=True)
    norm = jnp.sqrt(trace) + 1e-07
    a = gram / (norm * norm)
    q = None
    for sweep in range(ITERS):
        p = coef_a * eye + (coef_b * a + coef_c * mm(a, a))
        q = p if q is None else near(q, p)
        if sweep < ITERS - 1:
            a = mm(mm(a, p), p)
            yield q
    yield q / norm


def near(a, b):
    a_high, a_low = split(a)
    b_high, b_low = split(b)
    return dot(a_high, b_high) + (dot(a_high, b_low) + dot(a_low, b_high))


def dot(a, b):
    return jnp.dot(a, b, preferred_element_type=jnp.float32)


def across(a, b):
    return lax.dot_general(a, b, (((0,), (0,)), ((), ())), preferred_element_type=jnp.float32)


HALF = HD // 2
EDGE = 8
FIRST = HALF + EDGE
PIECES = FIRST + HALF
A = pl.ds(0, FIRST)
B = pl.ds(FIRST, HALF)


def grid_of_half():
    return lax.broadcasted_iota(jnp.int32, (HALF, HALF), 0), lax.broadcasted_iota(jnp.int32, (HALF, HALF), 1)


def store_packed(ref, lower, upper, diagonal, off):
    row, col = grid_of_half()
    ref[pl.ds(0, HALF), :] = jnp.where(row >= col, lower, upper)
    edge = jnp.sum(jnp.where(row == col, diagonal, 0.0), axis=0, keepdims=True)
    ref[pl.ds(HALF, EDGE), :] = jnp.broadcast_to(edge, (EDGE, HALF))
    ref[B, :] = off


def store_gram(ref, x):
    high = x.astype(jnp.bfloat16)
    rest = x - high.astype(jnp.float32)
    middle = rest.astype(jnp.bfloat16)
    low = (rest - middle.astype(jnp.float32)).astype(jnp.bfloat16)
    both = jnp.concatenate([high, middle], axis=0)
    even = across(both, both)
    half = across(jnp.concatenate([high, high], axis=0), jnp.concatenate([middle, low], axis=0))
    row, col = grid_of_half()
    h0, h1 = half[:HALF, :HALF], half[HALF:, HALF:]
    turned = jnp.where(row <= col, h0, h1).T
    e0, e1 = even[:HALF, :HALF], even[HALF:, HALF:]
    off = even[:HALF, HALF:] + (half[:HALF, HALF:] + half[HALF:, :HALF].T)
    store_packed(ref, e0 + h0 + turned, e1 + h1 + turned, e1 + 2.0 * h1, off)


def unpack(ref):
    row, col = grid_of_half()
    block, edge, off = ref[pl.ds(0, HALF), :], ref[pl.ds(HALF, 1), :], ref[B, :]
    turned = block.T
    first = jnp.where(row >= col, block, turned)
    second = jnp.where(row < col, block, jnp.where(row > col, turned, edge))
    return jnp.concatenate(
        [jnp.concatenate([first, off], axis=1), jnp.concatenate([off.T, second], axis=1)], axis=0
    )


def when(condition, action):
    if isinstance(condition, bool):
        if condition:
            action()
    else:
        pl.when(condition)(action)


def either(condition, first, second):
    if isinstance(condition, bool):
        (first if condition else second)()
    else:
        pl.when(condition)(first)
        pl.when(jnp.logical_not(condition))(second)


def run(pieces, count):
    for _ in range(count):
        next(pieces, None)


def toggle(index, flips, count):
    out, bit = 0, 1
    while bit < count:
        out = out + (index // bit + flips // bit) % 2 * bit
        bit *= 2
    return out


def exchange_kernel(
    devices, layers, limit, scale, g_hbm, m_hbm, w_hbm, new_w_ref, new_m_ref,
    g_ref, m_ref, w_ref, squares, mine, own, ra, ra2, rb, rb2, zr, q,
    square_send, square_recv, a1_send, a1_recv, b1_send, b1_recv, a2_send, a2_recv, b2_send, b2_recv,
    z_send, z_recv, ay_send, ay_recv, ax_send, ax_recv, bx_send, bx_recv, by_send, by_recv,
    qz_send, qz_recv, load_sem,
):
    rows, width = g_ref.shape
    heads = width // HD
    depth = devices // 4
    groups = heads // devices
    everyone = devices * layers
    me = lax.axis_index("rows")
    layer = lax.axis_index("layer")
    flat = me * layers + layer
    z, y, x = me // 4, me // 2 % 2, me % 2
    peer_x = z * 4 + y * 2 + (1 - x)
    peer_y = z * 4 + (1 - y) * 2 + x
    parts = load_sem.shape[0] - 2
    span = width // parts

    def load_g(i):
        cols = pl.ds(i * span, span)
        return pltpu.make_async_copy(g_hbm.at[:, cols], g_ref.at[:, cols], load_sem.at[2 + i])

    load_m = pltpu.make_async_copy(m_hbm, m_ref, load_sem.at[0])
    load_w = pltpu.make_async_copy(w_hbm, w_ref, load_sem.at[1])
    for i in range(parts):
        load_g(i).start()
    load_m.start()
    load_w.start()
    barrier = pltpu.get_barrier_semaphore()

    def other(k):
        peer = lax.rem(flat + k, everyone)
        return {"rows": lax.div(peer, layers), "layer": lax.rem(peer, layers)}

    for k in range(1, everyone):
        pl.semaphore_signal(barrier, inc=1, device_id=other(k), device_id_type=MESH)

    def columns_of(h):
        return pl.ds(pl.multiple_of(h * HD, HD), HD)

    def add_squares(h, acc):
        g = g_ref[:, columns_of(h)].astype(jnp.float32)
        return acc + (g * g).reshape(rows // 8, 8, HD).sum(axis=0)

    acc = jnp.zeros((8, HD), jnp.float32)
    for i in range(parts):
        load_g(i).wait()
        acc = lax.fori_loop(i * (heads // parts), (i + 1) * (heads // parts), add_squares, acc)
    part = acc[:, :128] + acc[:, 128:]
    mine[...] = part
    squares[flat] = part
    pl.semaphore_wait(barrier, everyone - 1)

    def square_copy(k):
        return pltpu.make_async_remote_copy(
            src_ref=mine,
            dst_ref=squares.at[flat],
            send_sem=square_send.at[k],
            recv_sem=square_recv.at[k],
            device_id=other(k),
            device_id_type=MESH,
        )

    for k in range(1, everyone):
        square_copy(k).start()
    for k in range(1, everyone):
        square_copy(k).wait_recv()

    total = jnp.sum(squares[...], axis=0)
    total = jnp.sum(jnp.sum(total, axis=0, keepdims=True), axis=1, keepdims=True)
    factor = jnp.minimum(1.0, limit / (jnp.sqrt(total) + 1e-06))
    load_m.wait()
    load_w.wait()

    def layer_of(k):
        return toggle(z, k, depth)

    def head_of(j, t, kind):
        owner = t * 4 + (y + kind % 2) % 2 * 2 + (x + kind // 2) % 2
        return owner * groups + j

    def send(src, dst, send_sem, recv_sem, device):
        return pltpu.make_async_remote_copy(
            src_ref=src, dst_ref=dst, send_sem=send_sem, recv_sem=recv_sem,
            device_id={"rows": device}, device_id_type=MESH,
        )

    def a1(j, t, dy):
        return send(own.at[j, t, 2 + dy, A], ra.at[j, t, dy], a1_send.at[j, t, dy], a1_recv.at[j, t, dy], peer_x)

    def b1(j, t, dx):
        return send(own.at[j, t, 2 * dx + 1, B], rb.at[j, t, dx], b1_send.at[j, t, dx], b1_recv.at[j, t, dx], peer_y)

    def a2(j, t):
        return send(own.at[j, t, 1, A], ra2.at[j, t], a2_send.at[j, t], a2_recv.at[j, t], peer_y)

    def b2(j, t):
        return send(own.at[j, t, 2, B], rb2.at[j, t], b2_send.at[j, t], b2_recv.at[j, t], peer_x)

    def zc(j, k):
        t = layer_of(k)
        return send(own.at[j, t, 0], zr.at[j, z], z_send.at[j, k], z_recv.at[j, k], t * 4 + y * 2 + x)

    def qz(j, k):
        t = layer_of(k)
        return send(q.at[j, z, 0], q.at[j, z, 0], qz_send.at[j, k], qz_recv.at[j, k], t * 4 + y * 2 + x)

    def ay(j, t):
        return send(q.at[j, t, 0, A], q.at[j, t, 1, A], ay_send.at[j, t], ay_recv.at[j, t], peer_y)

    def ax(j, t, dy):
        return send(q.at[j, t, dy, A], q.at[j, t, 2 + dy, A], ax_send.at[j, t, dy], ax_recv.at[j, t, dy], peer_x)

    def bx(j, t):
        return send(q.at[j, t, 0, B], q.at[j, t, 2, B], bx_send.at[j, t], bx_recv.at[j, t], peer_x)

    def by(j, t, dx):
        return send(
            q.at[j, t, 2 * dx, B], q.at[j, t, 2 * dx + 1, B], by_send.at[j, t, dx], by_recv.at[j, t, dx], peer_y
        )

    def first_send(j, k):
        t = layer_of(k)
        for kind in (3, 2, 1, 0):
            cols = columns_of(head_of(j, t, kind))
            clipped = factor * g_ref[:, cols].astype(jnp.float32)
            new_momentum = momentum_decay * m_ref[:, cols] + clipped
            new_m_ref[:, cols] = new_momentum
            store_gram(own.at[j, t, kind], clipped + momentum_decay * new_momentum)
        for half in (1, 0):
            a1(j, t, half).start()
            b1(j, t, half).start()

    def second_send(j, k):
        t = layer_of(k)
        a1(j, t, 1).wait_recv()
        own[j, t, 1, A, :] += ra[j, t, 1]
        a2(j, t).start()
        b1(j, t, 1).wait_recv()
        own[j, t, 2, B, :] += rb[j, t, 1]
        b2(j, t).start()

    def third_send(j, k):
        t = layer_of(k)
        a1(j, t, 0).wait_recv()
        b1(j, t, 0).wait_recv()
        a2(j, t).wait_recv()
        b2(j, t).wait_recv()
        a = own[j, t, 0, A, :] + (ra[j, t, 0] + ra2[j, t])
        b = own[j, t, 0, B, :] + (rb[j, t, 0] + rb2[j, t])

        def keep():
            zr[j, t, A, :] = a
            zr[j, t, B, :] = b

        def pass_up():
            own[j, t, 0, A, :] = a
            own[j, t, 0, B, :] = b
            zc(j, k).start()

        either(k == 0, keep, pass_up)

    def solve(j):
        for k in range(1, depth):
            zc(j, k).wait_recv()
        own[j, z, 0] = jnp.sum(zr[j], axis=0)
        for p in polynomial(unpack(own.at[j, z, 0])):
            yield
        store_packed(q.at[j, z, 0], p[:HALF, :HALF], p[HALF:, HALF:], p[HALF:, HALF:], p[:HALF, HALF:])
        for k in range(1, depth):
            qz(j, k).start()
        pass_on(j, 0)

    def pass_on(j, k):
        t = layer_of(k)
        if not (isinstance(k, int) and k == 0):
            qz(j, k).wait_recv()
        ay(j, t).start()
        bx(j, t).start()
        ax(j, t, 0).start()
        by(j, t, 0).start()

    def pass_far(j, k):
        t = layer_of(k)
        ay(j, t).wait_recv()
        ax(j, t, 1).start()
        bx(j, t).wait_recv()
        by(j, t, 1).start()

    def finish(j, k):
        t = layer_of(k)
        by(j, t, 0).wait_recv()
        by(j, t, 1).wait_recv()
        ax(j, t, 0).wait_recv()
        ax(j, t, 1).wait_recv()
        for kind in range(4):
            cols = columns_of(head_of(j, t, kind))
            q_high, q_low = split(unpack(q.at[j, t, kind]))
            update = factor * g_ref[:, cols].astype(jnp.float32) + momentum_decay * new_m_ref[:, cols]
            high, low = split(update)
            ortho = dot(high, q_high) + (dot(low, q_high) + dot(high, q_low))
            w = w_ref[:, cols]
            new_w_ref[:, cols] = w - learn_rate * (scale * ortho + weight_decay * w)

    last = groups - 1
    steps = groups * depth

    def forward(s):
        def at(step, action):
            action(step // depth, depth - 1 - step % depth)

        when(s < steps, lambda: at(s, first_send))
        when((s >= 1) & (s < steps + 1), lambda: at(s - 1, second_send))
        when(s >= 2, lambda: at(s - 2, third_send))

    @pl.loop(0, depth + 2)
    def _(s):
        forward(s)

    for j in range(groups):
        pieces = solve(j)
        if j < last:
            for s in range((j + 1) * depth + 2, (j + 2) * depth + 2):
                run(pieces, 2)
                forward(s)
            run(pieces, ITERS + 1)
        else:
            if j > 0:
                for k in range(1, depth):
                    pass_on(j - 1, k)
                    pass_far(j - 1, k - 1)
                    run(pieces, 2)
            run(pieces, ITERS + 1)
            if j > 0:
                pass_far(j - 1, depth - 1)
        if 0 < j < last:
            for k in range(1, depth):
                pass_on(j - 1, k)
                pass_far(j - 1, k - 1)
            pass_far(j - 1, depth - 1)

    @pl.loop(1, depth)
    def _(k):
        pass_on(last, k)
        pass_far(last, k - 1)
        for j in range(last):
            finish(j, k - 1)

    for j in range(last):
        finish(j, depth - 1)
    pass_far(last, depth - 1)

    @pl.loop(0, depth)
    def _(k):
        finish(last, k)

    @pl.loop(0, groups)
    def _(j):
        @pl.loop(0, depth)
        def _(k):
            for c in (a1(j, k, 0), a1(j, k, 1), b1(j, k, 0), b1(j, k, 1), a2(j, k), b2(j, k)):
                c.wait_send()
            for c in (ay(j, k), ax(j, k, 0), ax(j, k, 1), bx(j, k), by(j, k, 0), by(j, k, 1)):
                c.wait_send()

        @pl.loop(1, depth)
        def _(k):
            zc(j, k).wait_send()
            qz(j, k).wait_send()

    for k in range(1, everyone):
        square_copy(k).wait_send()


def exchange(gradient, momentum, weights, devices, layers, limit, scale):
    rows, width = gradient.shape
    heads = width // HD
    depth = devices // 4
    groups = heads // devices
    everyone = devices * layers
    vmem = lambda *shape: pltpu.VMEM(shape, jnp.float32)
    pair = lambda *shape: [pltpu.SemaphoreType.DMA(shape)] * 2
    one, two = (groups, depth), (groups, depth, 2)
    return pl.pallas_call(
        functools.partial(exchange_kernel, devices, layers, limit, scale),
        out_shape=(
            jax.ShapeDtypeStruct((rows, width), jnp.float32),
            jax.ShapeDtypeStruct((rows, width), jnp.float32),
        ),
        in_specs=[pl.BlockSpec(memory_space=pl.ANY)] * 3,
        out_specs=(pl.BlockSpec(memory_space=pltpu.VMEM), pl.BlockSpec(memory_space=pltpu.VMEM)),
        scratch_shapes=[
            pltpu.VMEM((rows, width), gradient.dtype),
            vmem(rows, width),
            vmem(rows, width),
            vmem(everyone, 8, 128),
            vmem(8, 128),
            vmem(groups, depth, 4, PIECES, HALF),
            vmem(groups, depth, 2, FIRST, HALF),
            vmem(groups, depth, FIRST, HALF),
            vmem(groups, depth, 2, HALF, HALF),
            vmem(groups, depth, HALF, HALF),
            vmem(groups, depth, PIECES, HALF),
            vmem(groups, depth, 4, PIECES, HALF),
            *pair(everyone),
            *pair(*two), *pair(*two), *pair(*one), *pair(*one), *pair(*one),
            *pair(*one), *pair(*two), *pair(*one), *pair(*two), *pair(*one),
            pltpu.SemaphoreType.DMA((2 + math.gcd(heads, 4),)),
        ],
        compiler_params=pltpu.CompilerParams(
            collective_id=0, has_side_effects=True, vmem_limit_bytes=56 * 1024 * 1024
        ),
    )(gradient, momentum, weights)


def body(grads, momentum, weights):
    devices, layers = lax.axis_size("rows"), lax.axis_size("layer")
    rows, width = grads.shape[1:]
    limit = 0.5 * math.sqrt(float(layers * devices * rows * width))
    scale = 0.2 * math.sqrt(float(max(devices * rows, HD)))
    new_weights, new_momentum = exchange(grads[0], momentum[0], weights[0], devices, layers, limit, scale)
    return (new_weights[None], new_momentum[None])


def shared_body(grads, momentum, weights):
    devices = lax.axis_size("rows")
    rows, width = grads.shape[1:]
    heads = width // HD
    gradient = grads[0].astype(jnp.float32)
    total = lax.psum(jnp.sum(gradient * gradient), ("rows", "layer"))
    limit = 0.5 * math.sqrt(float(lax.axis_size("layer") * devices * rows * width))
    factor = jnp.minimum(1.0, limit / (jnp.sqrt(total) + 1e-06))
    clipped = factor * gradient
    new_momentum = momentum_decay * momentum[0] + clipped
    update = clipped + momentum_decay * new_momentum
    sharers = devices // heads
    part = rows // sharers
    head_major = update.reshape(rows, heads, HD).transpose(1, 0, 2)
    outgoing = jnp.concatenate([head_major] * sharers, axis=0)
    pieces = lax.all_to_all(outgoing, "rows", split_axis=0, concat_axis=1, tiled=True)
    x = pieces[0]
    gram = lax.dot_general(x, x, (((0,), (0,)), ((), ())), precision=HIGHEST)
    *_, p = polynomial(gram)
    result = mm(x, p)
    side = lax.axis_index("rows") // heads
    shares = result.reshape(devices, sharers, part, HD)
    chosen = lax.dynamic_index_in_dim(shares, side, 1, keepdims=False)
    returned = lax.all_to_all(chosen, "rows", split_axis=0, concat_axis=0, tiled=True)
    returned = returned.reshape(sharers, heads, part, HD).transpose(0, 2, 1, 3).reshape(rows, width)
    scale = 0.2 * math.sqrt(float(max(devices * rows, HD)))
    new_weights = weights[0] - learn_rate * (scale * returned + weight_decay * weights[0])
    return (new_weights[None], new_momentum[None])


def solution(mesh):
    placed = P("layer", "rows", None)

    def step(grads, momentum, weights):
        heads = grads.shape[2] // HD
        devices = mesh.shape["rows"]
        depth = devices // 4
        direct = heads % devices == 0 and devices == 4 * depth and depth & (depth - 1) == 0
        chosen = body if direct else shared_body
        return jax.shard_map(
            chosen, mesh=mesh, in_specs=(placed,) * 3, out_specs=(placed, placed), check_vma=False
        )(grads, momentum, weights)

    return step
```

```python
import functools
import math

import jax
import jax.numpy as jnp
from jax import lax
from jax.experimental import pallas as pl
from jax.experimental.pallas import tpu as pltpu
from jax.sharding import PartitionSpec as P

HD = 256
ITERS = 5

coef_a = 3.4445
coef_b = -4.775
coef_c = 2.0315
momentum_decay = 0.95
learn_rate = 0.5
weight_decay = 0.1

HIGHEST = lax.Precision.HIGHEST
MESH = pl.DeviceIdType.MESH


def mm(a, b):
    return jnp.dot(a, b, precision=HIGHEST, preferred_element_type=jnp.float32)


def split(x):
    high = x.astype(jnp.bfloat16)
    low = (x - high.astype(jnp.float32)).astype(jnp.bfloat16)
    return high, low


def polynomial(gram):
    row = lax.broadcasted_iota(jnp.int32, (HD, HD), 0)
    col = lax.broadcasted_iota(jnp.int32, (HD, HD), 1)
    eye = jnp.where(row == col, 1.0, 0.0).astype(jnp.float32)
    trace = jnp.sum(jnp.sum(gram * eye, axis=0, keepdims=True), axis=1, keepdims=True)
    norm = jnp.sqrt(trace) + 1e-07
    a = gram / (norm * norm)
    q = None
    for sweep in range(ITERS):
        p = coef_a * eye + (coef_b * a + coef_c * near(a, a))
        q = p if q is None else near(q, p)
        if sweep < ITERS - 1:
            product = mm if sweep < ITERS - 3 else near
            a = product(product(a, p), p)
            yield q
    yield q / norm


def near(a, b):
    a_high, a_low = split(a)
    b_high, b_low = split(b)
    return dot(a_high, b_high) + (dot(a_high, b_low) + dot(a_low, b_high))


def dot(a, b):
    return jnp.dot(a, b, preferred_element_type=jnp.float32)


def across(a, b):
    return lax.dot_general(a, b, (((0,), (0,)), ((), ())), preferred_element_type=jnp.float32)


HALF = HD // 2
PACE = (3, 3)
EARLY = 2
EACH = 2
EDGE = 8
FIRST = HALF + EDGE
PIECES = FIRST + HALF
B = pl.ds(0, HALF)
A = pl.ds(HALF, HALF + 1)
BOTH = pl.ds(HALF, HALF)
LINE = pl.ds(2 * HALF, 1)
ALL = pl.ds(0, 2 * HALF + 1)
ONLY_A = pl.ds(0, HALF + 1)


def grid_of_half():
    return lax.broadcasted_iota(jnp.int32, (HALF, HALF), 0), lax.broadcasted_iota(jnp.int32, (HALF, HALF), 1)


def store_packed(ref, lower, upper, diagonal, off):
    row, col = grid_of_half()
    ref[BOTH, :] = jnp.where(row >= col, lower, upper)
    ref[LINE, :] = jnp.sum(jnp.where(row == col, diagonal, 0.0), axis=0, keepdims=True)
    ref[B, :] = off


def store_gram(ref, x):
    high = x.astype(jnp.bfloat16)
    rest = x - high.astype(jnp.float32)
    middle = rest.astype(jnp.bfloat16)
    low = (rest - middle.astype(jnp.float32)).astype(jnp.bfloat16)
    both = jnp.concatenate([high, middle], axis=0)
    even = across(both, both)
    half = across(jnp.concatenate([high, high], axis=0), jnp.concatenate([middle, low], axis=0))
    row, col = grid_of_half()
    h0, h1 = half[:HALF, :HALF], half[HALF:, HALF:]
    turned = jnp.where(row <= col, h0, h1).T
    e0, e1 = even[:HALF, :HALF], even[HALF:, HALF:]
    off = even[:HALF, HALF:] + (half[:HALF, HALF:] + half[HALF:, :HALF].T)
    store_packed(ref, e0 + h0 + turned, e1 + h1 + turned, e1 + 2.0 * h1, off)


def unpack(ref):
    row, col = grid_of_half()
    block, edge, off = ref[BOTH, :], ref[LINE, :], ref[B, :]
    turned = block.T
    first = jnp.where(row >= col, block, turned)
    second = jnp.where(row < col, block, jnp.where(row > col, turned, edge))
    return jnp.concatenate(
        [jnp.concatenate([first, off], axis=1), jnp.concatenate([off.T, second], axis=1)], axis=0
    )


def when(condition, action):
    if isinstance(condition, bool):
        if condition:
            action()
    else:
        pl.when(condition)(action)


def either(condition, first, second):
    if isinstance(condition, bool):
        (first if condition else second)()
    else:
        pl.when(condition)(first)
        pl.when(jnp.logical_not(condition))(second)


def run(pieces, count):
    for _ in range(count):
        next(pieces, None)


def toggle(index, flips, count):
    out, bit = 0, 1
    while bit < count:
        out = out + (index // bit + flips // bit) % 2 * bit
        bit *= 2
    return out


def exchange_kernel(
    devices, layers, limit, scale, g_hbm, m_hbm, w_hbm, new_w_ref, new_m_ref,
    g_ref, m_ref, w_ref, squares, mine, own, ra, ra2, rb, rb2, zr, q,
    square_send, square_recv, a1_send, a1_recv, b1_send, b1_recv, a2_send, a2_recv, b2_send, b2_recv,
    z_send, z_recv, ay_send, ay_recv, ax_send, ax_recv, bx_send, bx_recv, by_send, by_recv,
    qz_send, qz_recv, load_sem,
):
    rows, width = g_ref.shape
    heads = width // HD
    depth = devices // 4
    groups = heads // devices
    everyone = devices * layers
    me = lax.axis_index("rows")
    layer = lax.axis_index("layer")
    flat = me * layers + layer
    z, y, x = me // 4, me // 2 % 2, me % 2
    peer_x = z * 4 + y * 2 + (1 - x)
    peer_y = z * 4 + (1 - y) * 2 + x
    parts = load_sem.shape[0] - 2
    span = width // parts

    def load_g(i):
        cols = pl.ds(i * span, span)
        return pltpu.make_async_copy(g_hbm.at[:, cols], g_ref.at[:, cols], load_sem.at[2 + i])

    load_m = pltpu.make_async_copy(m_hbm, m_ref, load_sem.at[0])
    load_w = pltpu.make_async_copy(w_hbm, w_ref, load_sem.at[1])
    for i in range(parts):
        load_g(i).start()
    load_m.start()
    load_w.start()
    barrier = pltpu.get_barrier_semaphore()

    def other(k):
        peer = lax.rem(flat + k, everyone)
        return {"rows": lax.div(peer, layers), "layer": lax.rem(peer, layers)}

    for k in range(1, everyone):
        pl.semaphore_signal(barrier, inc=1, device_id=other(k), device_id_type=MESH)

    def columns_of(h):
        return pl.ds(pl.multiple_of(h * HD, HD), HD)

    def add_squares(h, acc):
        g = g_ref[:, columns_of(h)].astype(jnp.float32)
        return acc + (g * g).reshape(rows // 8, 8, HD).sum(axis=0)

    acc = jnp.zeros((8, HD), jnp.float32)
    for i in range(parts):
        load_g(i).wait()
        acc = lax.fori_loop(i * (heads // parts), (i + 1) * (heads // parts), add_squares, acc)
    part = acc[:, :128] + acc[:, 128:]
    mine[...] = part
    squares[flat] = part
    pl.semaphore_wait(barrier, everyone - 1)

    def square_copy(k):
        return pltpu.make_async_remote_copy(
            src_ref=mine,
            dst_ref=squares.at[flat],
            send_sem=square_send.at[k],
            recv_sem=square_recv.at[k],
            device_id=other(k),
            device_id_type=MESH,
        )

    for k in range(1, everyone):
        square_copy(k).start()
    for k in range(1, everyone):
        square_copy(k).wait_recv()

    total = jnp.sum(squares[...], axis=0)
    total = jnp.sum(jnp.sum(total, axis=0, keepdims=True), axis=1, keepdims=True)
    factor = jnp.minimum(1.0, limit / (jnp.sqrt(total) + 1e-06))
    load_m.wait()
    load_w.wait()

    def layer_of(k):
        return toggle(z, k, depth)

    def head_of(j, t, kind):
        owner = t * 4 + (y + kind % 2) % 2 * 2 + (x + kind // 2) % 2
        return owner * groups + j

    def send(src, dst, send_sem, recv_sem, device):
        return pltpu.make_async_remote_copy(
            src_ref=src, dst_ref=dst, send_sem=send_sem, recv_sem=recv_sem,
            device_id={"rows": device}, device_id_type=MESH,
        )

    def a1(j, t, dy):
        return send(own.at[j, t, 2 + dy, A], ra.at[j, t, dy, ONLY_A], a1_send.at[j, t, dy], a1_recv.at[j, t, dy], peer_x)

    def b1(j, t, dx):
        return send(own.at[j, t, 2 * dx + 1, B], rb.at[j, t, dx], b1_send.at[j, t, dx], b1_recv.at[j, t, dx], peer_y)

    def a2(j, t):
        return send(own.at[j, t, 1, A], ra2.at[j, t, ONLY_A], a2_send.at[j, t], a2_recv.at[j, t], peer_y)

    def b2(j, t):
        return send(own.at[j, t, 2, B], rb2.at[j, t], b2_send.at[j, t], b2_recv.at[j, t], peer_x)

    def zc(j, k):
        t = layer_of(k)
        return send(own.at[j, t, 0, ALL], zr.at[j, z, ALL], z_send.at[j, k], z_recv.at[j, k], t * 4 + y * 2 + x)

    def nearest(i):
        mirrored = 2 * z >= depth
        low = jnp.where(mirrored, depth - 1 - z, z)
        found = jnp.where(i > 2 * low, i, jnp.where(i % 2 == 1, low - (i + 1) // 2, low + i // 2))
        return jnp.where(mirrored, depth - 1 - found, found)

    def q_up(j, t):
        return send(q.at[j, t, 0, ALL], q.at[j, t, 0, ALL], qz_send.at[j, t, 0], qz_recv.at[j, t], (me + 4) % devices)

    def q_down(j, t):
        return send(q.at[j, t, 0, ALL], q.at[j, t, 0, ALL], qz_send.at[j, t, 1], qz_recv.at[j, t], (me + devices - 4) % devices)

    def ay(j, t):
        return send(q.at[j, t, 0, A], q.at[j, t, 1, A], ay_send.at[j, t], ay_recv.at[j, t], peer_y)

    def ax(j, t, dy):
        return send(q.at[j, t, dy, A], q.at[j, t, 2 + dy, A], ax_send.at[j, t, dy], ax_recv.at[j, t, dy], peer_x)

    def bx(j, t):
        return send(q.at[j, t, 0, B], q.at[j, t, 2, B], bx_send.at[j, t], bx_recv.at[j, t], peer_x)

    def by(j, t, dx):
        return send(
            q.at[j, t, 2 * dx, B], q.at[j, t, 2 * dx + 1, B], by_send.at[j, t, dx], by_recv.at[j, t, dx], peer_y
        )

    def first_send(j, k):
        t = layer_of(k)
        for kind in (3, 2, 1, 0):
            cols = columns_of(head_of(j, t, kind))
            clipped = factor * g_ref[:, cols].astype(jnp.float32)
            new_momentum = momentum_decay * m_ref[:, cols] + clipped
            new_m_ref[:, cols] = new_momentum
            store_gram(own.at[j, t, kind], clipped + momentum_decay * new_momentum)
            if kind == 3:
                a1(j, t, 1).start()
                b1(j, t, 1).start()
        a1(j, t, 0).start()
        b1(j, t, 0).start()

    def second_send(j, k):
        t = layer_of(k)
        a1(j, t, 1).wait_recv()
        own[j, t, 1, A, :] += ra[j, t, 1, ONLY_A, :]
        a2(j, t).start()
        b1(j, t, 1).wait_recv()
        own[j, t, 2, B, :] += rb[j, t, 1]
        b2(j, t).start()

    def third_send(j, k):
        t = layer_of(k)
        a1(j, t, 0).wait_recv()
        b1(j, t, 0).wait_recv()
        a2(j, t).wait_recv()
        b2(j, t).wait_recv()
        a = own[j, t, 0, A, :] + (ra[j, t, 0, ONLY_A, :] + ra2[j, t, ONLY_A, :])
        b = own[j, t, 0, B, :] + (rb[j, t, 0] + rb2[j, t])

        def keep():
            zr[j, t, A, :] = a
            zr[j, t, B, :] = b

        def pass_up():
            own[j, t, 0, A, :] = a
            own[j, t, 0, B, :] = b
            zc(j, k).start()

        either(k == 0, keep, pass_up)

    def solve(j):
        for k in range(1, depth):
            zc(j, k).wait_recv()
        own[j, z, 0, ALL, :] = jnp.sum(zr[j, :, ALL, :], axis=0)
        for p in polynomial(unpack(own.at[j, z, 0])):
            yield
        store_packed(q.at[j, z, 0], p[:HALF, :HALF], p[HALF:, HALF:], p[HALF:, HALF:], p[:HALF, HALF:])
        pass_on(j, 0)

    def pass_on(j, k):
        t = nearest(k)
        if not (isinstance(k, int) and k == 0):
            q_up(j, t).wait_recv()
        pl.when((z >= t) & (z < depth - 1))(lambda: q_up(j, t).start())
        pl.when((z <= t) & (z > 0))(lambda: q_down(j, t).start())
        ay(j, t).start()
        bx(j, t).start()
        ax(j, t, 0).start()
        by(j, t, 0).start()

    def pass_far(j, k):
        t = nearest(k)
        ay(j, t).wait_recv()
        ax(j, t, 1).start()
        bx(j, t).wait_recv()
        by(j, t, 1).start()

    def finish(j, k):
        t = nearest(k)
        by(j, t, 0).wait_recv()
        ax(j, t, 0).wait_recv()
        for kind in range(4):
            if kind == 3:
                by(j, t, 1).wait_recv()
                ax(j, t, 1).wait_recv()
            cols = columns_of(head_of(j, t, kind))
            q_high, q_low = split(unpack(q.at[j, t, kind]))
            update = factor * g_ref[:, cols].astype(jnp.float32) + momentum_decay * new_m_ref[:, cols]
            high, low = split(update)
            ortho = dot(high, q_high) + (dot(low, q_high) + dot(high, q_low))
            w = w_ref[:, cols]
            new_w_ref[:, cols] = w - learn_rate * (scale * ortho + weight_decay * w)

    last = groups - 1
    steps = groups * depth

    def forward(s):
        def at(step, action):
            action(step // depth, depth - 1 - step % depth)

        when(s < steps, lambda: at(s, first_send))
        when((s >= 1) & (s < steps + 1), lambda: at(s - 1, second_send))
        when(s >= 2, lambda: at(s - 2, third_send))

    @pl.loop(0, depth + 2)
    def _(s):
        forward(s)

    for j in range(groups):
        pieces = solve(j)
        if j < last:
            for s in range((j + 1) * depth + 2, (j + 2) * depth + 2):
                run(pieces, EACH)
                forward(s)
            run(pieces, ITERS + 1)
        else:
            if j > 0:
                for k in range(1, depth):
                    pass_on(j - 1, k)
                    pass_far(j - 1, k - 1)
                    run(pieces, PACE[min(k, len(PACE)) - 1])
            run(pieces, ITERS + 1)
            if j > 0:
                pass_far(j - 1, depth - 1)
        if 0 < j < last:
            for k in range(1, depth):
                pass_on(j - 1, k)
                pass_far(j - 1, k - 1)
            pass_far(j - 1, depth - 1)

    @pl.loop(1, depth)
    def _(k):
        pass_on(last, k)
        pass_far(last, k - 1)
        for j in range(last):
            finish(j, k - 1)
        pl.when(k > EARLY)(lambda: finish(last, k - 1 - EARLY))

    for j in range(last):
        finish(j, depth - 1)
    pass_far(last, depth - 1)

    @pl.loop(max(depth - 1 - EARLY, 0), depth)
    def _(k):
        finish(last, k)

    @pl.loop(0, groups)
    def _(j):
        @pl.loop(0, depth)
        def _(k):
            for c in (a1(j, k, 0), a1(j, k, 1), b1(j, k, 0), b1(j, k, 1), a2(j, k), b2(j, k)):
                c.wait_send()
            for c in (ay(j, k), ax(j, k, 0), ax(j, k, 1), bx(j, k), by(j, k, 0), by(j, k, 1)):
                c.wait_send()

            pl.when((z >= k) & (z < depth - 1))(lambda: q_up(j, k).wait_send())
            pl.when((z <= k) & (z > 0))(lambda: q_down(j, k).wait_send())

        @pl.loop(1, depth)
        def _(k):
            zc(j, k).wait_send()

    for k in range(1, everyone):
        square_copy(k).wait_send()


def exchange(gradient, momentum, weights, devices, layers, limit, scale):
    rows, width = gradient.shape
    heads = width // HD
    depth = devices // 4
    groups = heads // devices
    everyone = devices * layers
    vmem = lambda *shape: pltpu.VMEM(shape, jnp.float32)
    dma = pltpu.SemaphoreType.DMA
    pair = lambda *shape: [dma(shape)] * 2
    one, two = (groups, depth), (groups, depth, 2)
    return pl.pallas_call(
        functools.partial(exchange_kernel, devices, layers, limit, scale),
        out_shape=(
            jax.ShapeDtypeStruct((rows, width), jnp.float32),
            jax.ShapeDtypeStruct((rows, width), jnp.float32),
        ),
        in_specs=[pl.BlockSpec(memory_space=pl.ANY)] * 3,
        out_specs=(pl.BlockSpec(memory_space=pltpu.VMEM), pl.BlockSpec(memory_space=pltpu.VMEM)),
        scratch_shapes=[
            pltpu.VMEM((rows, width), gradient.dtype),
            vmem(rows, width),
            vmem(rows, width),
            vmem(everyone, 8, 128),
            vmem(8, 128),
            vmem(groups, depth, 4, PIECES, HALF),
            vmem(groups, depth, 2, FIRST, HALF),
            vmem(groups, depth, FIRST, HALF),
            vmem(groups, depth, 2, HALF, HALF),
            vmem(groups, depth, HALF, HALF),
            vmem(groups, depth, PIECES, HALF),
            vmem(groups, depth, 4, PIECES, HALF),
            *pair(everyone),
            *pair(*two), *pair(*two), *pair(*one), *pair(*one), *pair(*one),
            *pair(*one), *pair(*two), *pair(*one), *pair(*two), dma(two), dma(one),
            pltpu.SemaphoreType.DMA((2 + math.gcd(heads, 4),)),
        ],
        compiler_params=pltpu.CompilerParams(
            collective_id=0, has_side_effects=True, vmem_limit_bytes=56 * 1024 * 1024
        ),
    )(gradient, momentum, weights)


def body(grads, momentum, weights):
    devices, layers = lax.axis_size("rows"), lax.axis_size("layer")
    rows, width = grads.shape[1:]
    limit = 0.5 * math.sqrt(float(layers * devices * rows * width))
    scale = 0.2 * math.sqrt(float(max(devices * rows, HD)))
    new_weights, new_momentum = exchange(grads[0], momentum[0], weights[0], devices, layers, limit, scale)
    return (new_weights[None], new_momentum[None])


def shared_body(grads, momentum, weights):
    devices = lax.axis_size("rows")
    rows, width = grads.shape[1:]
    heads = width // HD
    gradient = grads[0].astype(jnp.float32)
    total = lax.psum(jnp.sum(gradient * gradient), ("rows", "layer"))
    limit = 0.5 * math.sqrt(float(lax.axis_size("layer") * devices * rows * width))
    factor = jnp.minimum(1.0, limit / (jnp.sqrt(total) + 1e-06))
    clipped = factor * gradient
    new_momentum = momentum_decay * momentum[0] + clipped
    update = clipped + momentum_decay * new_momentum
    sharers = devices // heads
    part = rows // sharers
    head_major = update.reshape(rows, heads, HD).transpose(1, 0, 2)
    outgoing = jnp.concatenate([head_major] * sharers, axis=0)
    pieces = lax.all_to_all(outgoing, "rows", split_axis=0, concat_axis=1, tiled=True)
    x = pieces[0]
    gram = lax.dot_general(x, x, (((0,), (0,)), ((), ())), precision=HIGHEST)
    *_, p = polynomial(gram)
    result = mm(x, p)
    side = lax.axis_index("rows") // heads
    shares = result.reshape(devices, sharers, part, HD)
    chosen = lax.dynamic_index_in_dim(shares, side, 1, keepdims=False)
    returned = lax.all_to_all(chosen, "rows", split_axis=0, concat_axis=0, tiled=True)
    returned = returned.reshape(sharers, heads, part, HD).transpose(0, 2, 1, 3).reshape(rows, width)
    scale = 0.2 * math.sqrt(float(max(devices * rows, HD)))
    new_weights = weights[0] - learn_rate * (scale * returned + weight_decay * weights[0])
    return (new_weights[None], new_momentum[None])


def solution(mesh):
    placed = P("layer", "rows", None)

    def step(grads, momentum, weights):
        heads = grads.shape[2] // HD
        devices = mesh.shape["rows"]
        depth = devices // 4
        direct = heads % devices == 0 and devices == 4 * depth and depth & (depth - 1) == 0
        chosen = body if direct else shared_body
        return jax.shard_map(
            chosen, mesh=mesh, in_specs=(placed,) * 3, out_specs=(placed, placed), check_vma=False
        )(grads, momentum, weights)

    return step
```

```python
import functools
import math

import jax
import jax.numpy as jnp
from jax import lax
from jax.experimental import pallas as pl
from jax.experimental.pallas import tpu as pltpu
from jax.sharding import PartitionSpec as P

HD = 256
ITERS = 5

coef_a = 3.4445
coef_b = -4.775
coef_c = 2.0315
momentum_decay = 0.95
learn_rate = 0.5
weight_decay = 0.1

HIGHEST = lax.Precision.HIGHEST
MESH = pl.DeviceIdType.MESH


def mm(a, b):
    return jnp.dot(a, b, precision=HIGHEST, preferred_element_type=jnp.float32)


def split(x):
    high = x.astype(jnp.bfloat16)
    low = (x - high.astype(jnp.float32)).astype(jnp.bfloat16)
    return high, low


def polynomial(gram):
    row = lax.broadcasted_iota(jnp.int32, (HD, HD), 0)
    col = lax.broadcasted_iota(jnp.int32, (HD, HD), 1)
    eye = jnp.where(row == col, 1.0, 0.0).astype(jnp.float32)
    trace = jnp.sum(jnp.sum(gram * eye, axis=0, keepdims=True), axis=1, keepdims=True)
    norm = jnp.sqrt(trace) + 1e-07
    a = gram / (norm * norm)
    q = None
    for sweep in range(ITERS):
        p = coef_a * eye + (coef_b * a + coef_c * near(a, a))
        q = p if q is None else near(q, p)
        if sweep < ITERS - 1:
            product = mm if sweep < ITERS - 2 else near
            a = product(product(a, p), p)
            yield q
    yield q / norm


def near(a, b):
    a_high, a_low = split(a)
    b_high, b_low = split(b)
    return dot(a_high, b_high) + (dot(a_high, b_low) + dot(a_low, b_high))


def dot(a, b):
    return jnp.dot(a, b, preferred_element_type=jnp.float32)


def across(a, b):
    return lax.dot_general(a, b, (((0,), (0,)), ((), ())), preferred_element_type=jnp.float32)


HALF = HD // 2
PACE = (2, 4)
EARLY = 2
EACH = 2
EDGE = 8
FIRST = HALF + EDGE
PIECES = FIRST + HALF
B = pl.ds(0, HALF)
A = pl.ds(HALF, HALF + 1)
BOTH = pl.ds(HALF, HALF)
LINE = pl.ds(2 * HALF, 1)
ALL = pl.ds(0, 2 * HALF + 1)
ONLY_A = pl.ds(0, HALF + 1)


def grid_of_half():
    return lax.broadcasted_iota(jnp.int32, (HALF, HALF), 0), lax.broadcasted_iota(jnp.int32, (HALF, HALF), 1)


def store_packed(ref, lower, upper, diagonal, off):
    row, col = grid_of_half()
    ref[BOTH, :] = jnp.where(row >= col, lower, upper)
    ref[LINE, :] = jnp.sum(jnp.where(row == col, diagonal, 0.0), axis=0, keepdims=True)
    ref[B, :] = off


def store_gram(ref, x):
    high = x.astype(jnp.bfloat16)
    rest = x - high.astype(jnp.float32)
    middle = rest.astype(jnp.bfloat16)
    low = (rest - middle.astype(jnp.float32)).astype(jnp.bfloat16)
    both = jnp.concatenate([high, middle], axis=0)
    even = across(both, both)
    half = across(jnp.concatenate([high, high], axis=0), jnp.concatenate([middle, low], axis=0))
    row, col = grid_of_half()
    h0, h1 = half[:HALF, :HALF], half[HALF:, HALF:]
    turned = jnp.where(row <= col, h0, h1).T
    e0, e1 = even[:HALF, :HALF], even[HALF:, HALF:]
    off = even[:HALF, HALF:] + (half[:HALF, HALF:] + half[HALF:, :HALF].T)
    store_packed(ref, e0 + h0 + turned, e1 + h1 + turned, e1 + 2.0 * h1, off)


def unpack(ref):
    row, col = grid_of_half()
    block, edge, off = ref[BOTH, :], ref[LINE, :], ref[B, :]
    turned = block.T
    first = jnp.where(row >= col, block, turned)
    second = jnp.where(row < col, block, jnp.where(row > col, turned, edge))
    return jnp.concatenate(
        [jnp.concatenate([first, off], axis=1), jnp.concatenate([off.T, second], axis=1)], axis=0
    )


def when(condition, action):
    if isinstance(condition, bool):
        if condition:
            action()
    else:
        pl.when(condition)(action)


def either(condition, first, second):
    if isinstance(condition, bool):
        (first if condition else second)()
    else:
        pl.when(condition)(first)
        pl.when(jnp.logical_not(condition))(second)


def run(pieces, count):
    for _ in range(count):
        next(pieces, None)


def toggle(index, flips, count):
    out, bit = 0, 1
    while bit < count:
        out = out + (index // bit + flips // bit) % 2 * bit
        bit *= 2
    return out


def exchange_kernel(
    devices, layers, limit, scale, g_hbm, m_hbm, w_hbm, new_w_ref, new_m_ref,
    g_ref, m_ref, w_ref, squares, mine, own, ra, ra2, rb, rb2, zr, q,
    square_send, square_recv, a1_send, a1_recv, b1_send, b1_recv, a2_send, a2_recv, b2_send, b2_recv,
    z_send, z_recv, ay_send, ay_recv, ax_send, ax_recv, bx_send, bx_recv, by_send, by_recv,
    qz_send, qz_recv, load_sem,
):
    rows, width = g_ref.shape
    heads = width // HD
    depth = devices // 4
    groups = heads // devices
    everyone = devices * layers
    me = lax.axis_index("rows")
    layer = lax.axis_index("layer")
    flat = me * layers + layer
    z, y, x = me // 4, me // 2 % 2, me % 2
    peer_x = z * 4 + y * 2 + (1 - x)
    peer_y = z * 4 + (1 - y) * 2 + x
    parts = load_sem.shape[0] - 2
    span = width // parts

    def load_g(i):
        cols = pl.ds(i * span, span)
        return pltpu.make_async_copy(g_hbm.at[:, cols], g_ref.at[:, cols], load_sem.at[2 + i])

    load_m = pltpu.make_async_copy(m_hbm, m_ref, load_sem.at[0])
    load_w = pltpu.make_async_copy(w_hbm, w_ref, load_sem.at[1])
    for i in range(parts):
        load_g(i).start()
    load_m.start()
    load_w.start()
    barrier = pltpu.get_barrier_semaphore()

    def other(k):
        peer = lax.rem(flat + k, everyone)
        return {"rows": lax.div(peer, layers), "layer": lax.rem(peer, layers)}

    for k in range(1, everyone):
        pl.semaphore_signal(barrier, inc=1, device_id=other(k), device_id_type=MESH)

    def columns_of(h):
        return pl.ds(pl.multiple_of(h * HD, HD), HD)

    def add_squares(h, acc):
        g = g_ref[:, columns_of(h)].astype(jnp.float32)
        return acc + (g * g).reshape(rows // 8, 8, HD).sum(axis=0)

    acc = jnp.zeros((8, HD), jnp.float32)
    for i in range(parts):
        load_g(i).wait()
        acc = lax.fori_loop(i * (heads // parts), (i + 1) * (heads // parts), add_squares, acc)
    part = acc[:, :128] + acc[:, 128:]
    mine[...] = part
    squares[flat] = part
    pl.semaphore_wait(barrier, everyone - 1)

    def square_copy(k):
        return pltpu.make_async_remote_copy(
            src_ref=mine,
            dst_ref=squares.at[flat],
            send_sem=square_send.at[k],
            recv_sem=square_recv.at[k],
            device_id=other(k),
            device_id_type=MESH,
        )

    for k in range(1, everyone):
        square_copy(k).start()
    for k in range(1, everyone):
        square_copy(k).wait_recv()

    total = jnp.sum(squares[...], axis=0)
    total = jnp.sum(jnp.sum(total, axis=0, keepdims=True), axis=1, keepdims=True)
    factor = jnp.minimum(1.0, limit / (jnp.sqrt(total) + 1e-06))
    load_m.wait()
    load_w.wait()

    def layer_of(k):
        return toggle(z, k, depth)

    def head_of(j, t, kind):
        owner = t * 4 + (y + kind % 2) % 2 * 2 + (x + kind // 2) % 2
        return owner * groups + j

    def send(src, dst, send_sem, recv_sem, device):
        return pltpu.make_async_remote_copy(
            src_ref=src, dst_ref=dst, send_sem=send_sem, recv_sem=recv_sem,
            device_id={"rows": device}, device_id_type=MESH,
        )

    def a1(j, t, dy):
        return send(own.at[j, t, 2 + dy, A], ra.at[j, t, dy, ONLY_A], a1_send.at[j, t, dy], a1_recv.at[j, t, dy], peer_x)

    def b1(j, t, dx):
        return send(own.at[j, t, 2 * dx + 1, B], rb.at[j, t, dx], b1_send.at[j, t, dx], b1_recv.at[j, t, dx], peer_y)

    def a2(j, t):
        return send(own.at[j, t, 1, A], ra2.at[j, t, ONLY_A], a2_send.at[j, t], a2_recv.at[j, t], peer_y)

    def b2(j, t):
        return send(own.at[j, t, 2, B], rb2.at[j, t], b2_send.at[j, t], b2_recv.at[j, t], peer_x)

    def zc(j, k):
        t = layer_of(k)
        return send(own.at[j, t, 0, ALL], zr.at[j, z, ALL], z_send.at[j, k], z_recv.at[j, k], t * 4 + y * 2 + x)

    def nearest(i):
        mirrored = 2 * z >= depth
        low = jnp.where(mirrored, depth - 1 - z, z)
        found = jnp.where(i > 2 * low, i, jnp.where(i % 2 == 1, low - (i + 1) // 2, low + i // 2))
        return jnp.where(mirrored, depth - 1 - found, found)

    def q_up(j, t):
        return send(q.at[j, t, 0, ALL], q.at[j, t, 0, ALL], qz_send.at[j, t, 0], qz_recv.at[j, t], (me + 4) % devices)

    def q_down(j, t):
        return send(q.at[j, t, 0, ALL], q.at[j, t, 0, ALL], qz_send.at[j, t, 1], qz_recv.at[j, t], (me + devices - 4) % devices)

    def ay(j, t):
        return send(q.at[j, t, 0, A], q.at[j, t, 1, A], ay_send.at[j, t], ay_recv.at[j, t], peer_y)

    def ax(j, t, dy):
        return send(q.at[j, t, dy, A], q.at[j, t, 2 + dy, A], ax_send.at[j, t, dy], ax_recv.at[j, t, dy], peer_x)

    def bx(j, t):
        return send(q.at[j, t, 0, B], q.at[j, t, 2, B], bx_send.at[j, t], bx_recv.at[j, t], peer_x)

    def by(j, t, dx):
        return send(
            q.at[j, t, 2 * dx, B], q.at[j, t, 2 * dx + 1, B], by_send.at[j, t, dx], by_recv.at[j, t, dx], peer_y
        )

    def first_send(j, k):
        t = layer_of(k)
        for kind in (3, 2, 1, 0):
            cols = columns_of(head_of(j, t, kind))
            clipped = factor * g_ref[:, cols].astype(jnp.float32)
            new_momentum = momentum_decay * m_ref[:, cols] + clipped
            new_m_ref[:, cols] = new_momentum
            store_gram(own.at[j, t, kind], clipped + momentum_decay * new_momentum)
            if kind == 3:
                a1(j, t, 1).start()
                b1(j, t, 1).start()
        a1(j, t, 0).start()
        b1(j, t, 0).start()

    def second_send(j, k):
        t = layer_of(k)
        a1(j, t, 1).wait_recv()
        own[j, t, 1, A, :] += ra[j, t, 1, ONLY_A, :]
        a2(j, t).start()
        b1(j, t, 1).wait_recv()
        own[j, t, 2, B, :] += rb[j, t, 1]
        b2(j, t).start()

    def third_send(j, k):
        t = layer_of(k)
        a1(j, t, 0).wait_recv()
        b1(j, t, 0).wait_recv()
        a2(j, t).wait_recv()
        b2(j, t).wait_recv()
        a = own[j, t, 0, A, :] + (ra[j, t, 0, ONLY_A, :] + ra2[j, t, ONLY_A, :])
        b = own[j, t, 0, B, :] + (rb[j, t, 0] + rb2[j, t])

        def keep():
            zr[j, t, A, :] = a
            zr[j, t, B, :] = b

        def pass_up():
            own[j, t, 0, A, :] = a
            own[j, t, 0, B, :] = b
            zc(j, k).start()

        either(k == 0, keep, pass_up)

    def solve(j):
        for k in range(1, depth):
            zc(j, k).wait_recv()
        own[j, z, 0, ALL, :] = jnp.sum(zr[j, :, ALL, :], axis=0)
        for p in polynomial(unpack(own.at[j, z, 0])):
            yield
        store_packed(q.at[j, z, 0], p[:HALF, :HALF], p[HALF:, HALF:], p[HALF:, HALF:], p[:HALF, HALF:])
        pass_on(j, 0)

    def pass_on(j, k):
        t = nearest(k)
        if not (isinstance(k, int) and k == 0):
            q_up(j, t).wait_recv()
        pl.when((z >= t) & (z < depth - 1))(lambda: q_up(j, t).start())
        pl.when((z <= t) & (z > 0))(lambda: q_down(j, t).start())
        ay(j, t).start()
        bx(j, t).start()
        ax(j, t, 0).start()
        by(j, t, 0).start()

    def pass_far(j, k):
        t = nearest(k)
        ay(j, t).wait_recv()
        ax(j, t, 1).start()
        bx(j, t).wait_recv()
        by(j, t, 1).start()

    def finish(j, k):
        t = nearest(k)
        by(j, t, 0).wait_recv()
        ax(j, t, 0).wait_recv()
        for kind in range(4):
            if kind == 3:
                by(j, t, 1).wait_recv()
                ax(j, t, 1).wait_recv()
            cols = columns_of(head_of(j, t, kind))
            q_high, q_low = split(unpack(q.at[j, t, kind]))
            update = factor * g_ref[:, cols].astype(jnp.float32) + momentum_decay * new_m_ref[:, cols]
            high, low = split(update)
            ortho = dot(high, q_high) + (dot(low, q_high) + dot(high, q_low))
            w = w_ref[:, cols]
            new_w_ref[:, cols] = w - learn_rate * (scale * ortho + weight_decay * w)

    last = groups - 1
    steps = groups * depth

    def forward(s):
        def at(step, action):
            action(step // depth, depth - 1 - step % depth)

        when((s >= 1) & (s < steps + 1), lambda: at(s - 1, second_send))
        when(s < steps, lambda: at(s, first_send))
        when(s >= 2, lambda: at(s - 2, third_send))

    @pl.loop(0, depth + 2)
    def _(s):
        forward(s)

    for j in range(groups):
        pieces = solve(j)
        if j < last:
            for s in range((j + 1) * depth + 2, (j + 2) * depth + 2):
                run(pieces, EACH)
                forward(s)
            run(pieces, ITERS + 1)
        else:
            if j > 0:
                for k in range(1, depth):
                    pass_on(j - 1, k)
                    pass_far(j - 1, k - 1)
                    run(pieces, PACE[min(k, len(PACE)) - 1])
            run(pieces, ITERS + 1)
            if j > 0:
                pass_far(j - 1, depth - 1)
        if 0 < j < last:
            for k in range(1, depth):
                pass_on(j - 1, k)
                pass_far(j - 1, k - 1)
            pass_far(j - 1, depth - 1)

    @pl.loop(1, depth)
    def _(k):
        pass_on(last, k)
        pass_far(last, k - 1)
        for j in range(last):
            finish(j, k - 1)
        pl.when(k > EARLY)(lambda: finish(last, k - 1 - EARLY))

    for j in range(last):
        finish(j, depth - 1)
    pass_far(last, depth - 1)

    @pl.loop(max(depth - 1 - EARLY, 0), depth)
    def _(k):
        finish(last, k)

    @pl.loop(0, groups)
    def _(j):
        @pl.loop(0, depth)
        def _(k):
            for c in (a1(j, k, 0), a1(j, k, 1), b1(j, k, 0), b1(j, k, 1), a2(j, k), b2(j, k)):
                c.wait_send()
            for c in (ay(j, k), ax(j, k, 0), ax(j, k, 1), bx(j, k), by(j, k, 0), by(j, k, 1)):
                c.wait_send()

            pl.when((z >= k) & (z < depth - 1))(lambda: q_up(j, k).wait_send())
            pl.when((z <= k) & (z > 0))(lambda: q_down(j, k).wait_send())

        @pl.loop(1, depth)
        def _(k):
            zc(j, k).wait_send()

    for k in range(1, everyone):
        square_copy(k).wait_send()


def exchange(gradient, momentum, weights, devices, layers, limit, scale):
    rows, width = gradient.shape
    heads = width // HD
    depth = devices // 4
    groups = heads // devices
    everyone = devices * layers
    vmem = lambda *shape: pltpu.VMEM(shape, jnp.float32)
    dma = pltpu.SemaphoreType.DMA
    pair = lambda *shape: [dma(shape)] * 2
    one, two = (groups, depth), (groups, depth, 2)
    return pl.pallas_call(
        functools.partial(exchange_kernel, devices, layers, limit, scale),
        out_shape=(
            jax.ShapeDtypeStruct((rows, width), jnp.float32),
            jax.ShapeDtypeStruct((rows, width), jnp.float32),
        ),
        in_specs=[pl.BlockSpec(memory_space=pl.ANY)] * 3,
        out_specs=(pl.BlockSpec(memory_space=pltpu.VMEM), pl.BlockSpec(memory_space=pltpu.VMEM)),
        scratch_shapes=[
            pltpu.VMEM((rows, width), gradient.dtype),
            vmem(rows, width),
            vmem(rows, width),
            vmem(everyone, 8, 128),
            vmem(8, 128),
            vmem(groups, depth, 4, PIECES, HALF),
            vmem(groups, depth, 2, FIRST, HALF),
            vmem(groups, depth, FIRST, HALF),
            vmem(groups, depth, 2, HALF, HALF),
            vmem(groups, depth, HALF, HALF),
            vmem(groups, depth, PIECES, HALF),
            vmem(groups, depth, 4, PIECES, HALF),
            *pair(everyone),
            *pair(*two), *pair(*two), *pair(*one), *pair(*one), *pair(*one),
            *pair(*one), *pair(*two), *pair(*one), *pair(*two), dma(two), dma(one),
            pltpu.SemaphoreType.DMA((2 + math.gcd(heads, 4),)),
        ],
        compiler_params=pltpu.CompilerParams(
            collective_id=0, has_side_effects=True, vmem_limit_bytes=56 * 1024 * 1024
        ),
    )(gradient, momentum, weights)


def body(grads, momentum, weights):
    devices, layers = lax.axis_size("rows"), lax.axis_size("layer")
    rows, width = grads.shape[1:]
    limit = 0.5 * math.sqrt(float(layers * devices * rows * width))
    scale = 0.2 * math.sqrt(float(max(devices * rows, HD)))
    new_weights, new_momentum = exchange(grads[0], momentum[0], weights[0], devices, layers, limit, scale)
    return (new_weights[None], new_momentum[None])


def shared_body(grads, momentum, weights):
    devices = lax.axis_size("rows")
    rows, width = grads.shape[1:]
    heads = width // HD
    gradient = grads[0].astype(jnp.float32)
    total = lax.psum(jnp.sum(gradient * gradient), ("rows", "layer"))
    limit = 0.5 * math.sqrt(float(lax.axis_size("layer") * devices * rows * width))
    factor = jnp.minimum(1.0, limit / (jnp.sqrt(total) + 1e-06))
    clipped = factor * gradient
    new_momentum = momentum_decay * momentum[0] + clipped
    update = clipped + momentum_decay * new_momentum
    sharers = devices // heads
    part = rows // sharers
    head_major = update.reshape(rows, heads, HD).transpose(1, 0, 2)
    outgoing = jnp.concatenate([head_major] * sharers, axis=0)
    pieces = lax.all_to_all(outgoing, "rows", split_axis=0, concat_axis=1, tiled=True)
    x = pieces[0]
    gram = lax.dot_general(x, x, (((0,), (0,)), ((), ())), precision=HIGHEST)
    *_, p = polynomial(gram)
    result = mm(x, p)
    side = lax.axis_index("rows") // heads
    shares = result.reshape(devices, sharers, part, HD)
    chosen = lax.dynamic_index_in_dim(shares, side, 1, keepdims=False)
    returned = lax.all_to_all(chosen, "rows", split_axis=0, concat_axis=0, tiled=True)
    returned = returned.reshape(sharers, heads, part, HD).transpose(0, 2, 1, 3).reshape(rows, width)
    scale = 0.2 * math.sqrt(float(max(devices * rows, HD)))
    new_weights = weights[0] - learn_rate * (scale * returned + weight_decay * weights[0])
    return (new_weights[None], new_momentum[None])


def solution(mesh):
    placed = P("layer", "rows", None)

    def step(grads, momentum, weights):
        heads = grads.shape[2] // HD
        devices = mesh.shape["rows"]
        depth = devices // 4
        direct = heads % devices == 0 and devices == 4 * depth and depth & (depth - 1) == 0
        chosen = body if direct else shared_body
        return jax.shard_map(
            chosen, mesh=mesh, in_specs=(placed,) * 3, out_specs=(placed, placed), check_vma=False
        )(grads, momentum, weights)

    return step
```
